8 devices in a mesh: dp: 1 (over z), tp: 2 (over y), cp: 4 (over x, core).
Axes of the slice: x: 2, y: 2, z: 1, core: 2. Of those that a mesh axis runs over, the one named last changes fastest.
Arguments:
- hidden_in: bfloat16 [4, 512, 4096], P('dp')
- lengths: int32 [4], P('dp')
- k_cache: bfloat16 [4, 32, 2048, 128], P('dp', 'tp', 'cp')
- v_cache: bfloat16 [4, 32, 2048, 128], P('dp', 'tp', 'cp')
- ln1_gain: float32 [4096], replicated
- ln1_bias: float32 [4096], replicated
- ln2_gain: float32 [4096], replicated
- ln2_bias: float32 [4096], replicated
- w_qkv: bfloat16 [4096, 12288], P(None, 'tp')
- b_qkv: bfloat16 [12288], P('tp')
- w_out: bfloat16 [4096, 4096], P('tp')
- b_out: bfloat16 [4096], replicated
- w_up: bfloat16 [4096, 16384], P(None, 'tp')
- b_up: bfloat16 [16384], P('tp')
- w_down: bfloat16 [16384, 4096], P('tp')
- b_down: bfloat16 [4096], replicated
Outputs:
- output 1: bfloat16 [4, 512, 4096], P('dp')
- output 2: bfloat16 [4, 32, 512, 128], P('dp', 'tp')
- output 3: bfloat16 [4, 32, 512, 128], P('dp', 'tp')
All inputs are finite; a program needn't handle non-finite values.
Results may differ from the reference program's by a relative error of at most 0.00424842.
Values sent between devices are 32-bit elements.
A program may use at most 1.25 GiB of HBM per device.

```python
import math
import jax
import jax.numpy as jnp
from jax import lax

D_MODEL = 4096
NUM_HEADS = 32
HEAD_DIM = 128
FF_DIM = 16384
NUM_ROWS = 4
CHUNK_LEN = 512
CACHE_LEN = 2048
ROT_DIM = HEAD_DIM // 4
SCORE_SCALE = HEAD_DIM ** -0.5
Q_SCALE = math.sqrt(math.log(CACHE_LEN / 4.0))
NEG_BIG = -1e30
EPSILON = 1e-5
ROPE_BASE = 10000.0


def draw_lengths(len_key):
    draw_keys = jax.random.split(len_key, 2)
    drawn = jax.random.randint(draw_keys[0], (NUM_ROWS,), 1, CACHE_LEN + 1, dtype=jnp.int32)
    full_row = jax.random.randint(draw_keys[1], (), 0, NUM_ROWS, dtype=jnp.int32)
    row_ids = jnp.arange(NUM_ROWS, dtype=jnp.int32)
    drawn = jnp.where(row_ids == full_row, CACHE_LEN, drawn)
    return jnp.where(row_ids == (full_row + 1) % NUM_ROWS, 1, drawn).astype(jnp.int32)


def draw_cache(cache_key):
    row_keys = jax.random.split(cache_key, NUM_ROWS)
    return lax.map(lambda row_key: jax.random.normal(row_key, (NUM_HEADS, CACHE_LEN, HEAD_DIM), jnp.float32).astype(jnp.bfloat16), row_keys)


def setup_inputs(seed: int = 0, part: int = 0) -> dict:
    shared = jax.random.split(jax.random.key(seed), 12)
    part_keys = jax.random.split(jax.random.fold_in(jax.random.key(seed + 1), part), 4)
    qkv_gain = jnp.array([Q_SCALE, 1.0, 1.0], jnp.float32).reshape(1, 3, 1)
    hidden_in = 0.5 * jax.random.normal(part_keys[0], (NUM_ROWS, CHUNK_LEN, D_MODEL), jnp.float32)
    w_qkv = jax.random.normal(shared[0], (D_MODEL, NUM_HEADS, 3, HEAD_DIM), jnp.float32) * qkv_gain * D_MODEL ** -0.5
    b_qkv = 0.5 * jax.random.normal(shared[1], (NUM_HEADS, 3, HEAD_DIM), jnp.float32) * qkv_gain
    return {
        "hidden_in": hidden_in.astype(jnp.bfloat16),
        "lengths": draw_lengths(part_keys[1]),
        "k_cache": draw_cache(part_keys[2]),
        "v_cache": draw_cache(part_keys[3]),
        "ln1_gain": 1.0 + 0.2 * jax.random.normal(shared[2], (D_MODEL,), jnp.float32),
        "ln1_bias": 0.2 * jax.random.normal(shared[3], (D_MODEL,), jnp.float32),
        "ln2_gain": 1.0 + 0.2 * jax.random.normal(shared[4], (D_MODEL,), jnp.float32),
        "ln2_bias": 0.2 * jax.random.normal(shared[5], (D_MODEL,), jnp.float32),
        "w_qkv": w_qkv.reshape(D_MODEL, NUM_HEADS * 3 * HEAD_DIM).astype(jnp.bfloat16),
        "b_qkv": b_qkv.reshape(NUM_HEADS * 3 * HEAD_DIM).astype(jnp.bfloat16),
        "w_out": (1.5 * D_MODEL ** -0.5 * jax.random.normal(shared[6], (D_MODEL, D_MODEL), jnp.float32)).astype(jnp.bfloat16),
        "b_out": (0.5 * jax.random.normal(shared[7], (D_MODEL,), jnp.float32)).astype(jnp.bfloat16),
        "w_up": (D_MODEL ** -0.5 * jax.random.normal(shared[8], (D_MODEL, FF_DIM), jnp.float32)).astype(jnp.bfloat16),
        "b_up": (0.5 * jax.random.normal(shared[9], (FF_DIM,), jnp.float32)).astype(jnp.bfloat16),
        "w_down": (FF_DIM ** -0.5 * jax.random.normal(shared[10], (FF_DIM, D_MODEL), jnp.float32)).astype(jnp.bfloat16),
        "b_down": (0.5 * jax.random.normal(shared[11], (D_MODEL,), jnp.float32)).astype(jnp.bfloat16),
    }


def layer_norm(values_in, gain_vec, bias_vec):
    x_f32 = values_in.astype(jnp.float32)
    row_mean = jnp.mean(x_f32, axis=-1, keepdims=True)
    centered = x_f32 - row_mean
    variance = jnp.mean(centered * centered, axis=-1, keepdims=True)
    return (centered * lax.rsqrt(variance + EPSILON) * gain_vec + bias_vec).astype(jnp.bfloat16)


def rotary(values_in, positions):
    half_rot = ROT_DIM // 2
    inv_freq = ROPE_BASE ** (-2.0 * jnp.arange(half_rot, dtype=jnp.float32) / ROT_DIM)
    angles = positions.astype(jnp.float32)[..., None] * inv_freq
    cos_tab = jnp.cos(angles)[..., None, :]
    sin_tab = jnp.sin(angles)[..., None, :]
    rot_first = values_in[..., :half_rot].astype(jnp.float32)
    rot_second = values_in[..., half_rot:ROT_DIM].astype(jnp.float32)
    new_first = rot_first * cos_tab - rot_second * sin_tab
    new_second = rot_second * cos_tab + rot_first * sin_tab
    return jnp.concatenate([new_first.astype(jnp.bfloat16), new_second.astype(jnp.bfloat16), values_in[..., ROT_DIM:]], axis=-1)


def attend_row(operands):
    q_row, kn_row, vn_row, kc_row, vc_row, row_len = operands
    cache_valid = (jnp.arange(CACHE_LEN) < row_len)[None, :]
    causal = jnp.arange(CHUNK_LEN)[:, None] >= jnp.arange(CHUNK_LEN)[None, :]

    def attend_head(head_ops):
        q_head, kn_head, vn_head, kc_head, vc_head = head_ops
        s_cache = jnp.where(cache_valid, jnp.dot(q_head, kc_head.T, preferred_element_type=jnp.float32) * SCORE_SCALE, NEG_BIG)
        s_self = jnp.where(causal, jnp.dot(q_head, kn_head.T, preferred_element_type=jnp.float32) * SCORE_SCALE, NEG_BIG)
        row_max = jnp.maximum(s_cache.max(axis=1), s_self.max(axis=1))[:, None]
        p_cache = jnp.where(cache_valid, jnp.exp(s_cache - row_max), 0.0)
        p_self = jnp.where(causal, jnp.exp(s_self - row_max), 0.0)
        prob_sum = p_cache.sum(axis=1) + p_self.sum(axis=1)
        weighted = jnp.dot(p_cache.astype(jnp.bfloat16), vc_head, preferred_element_type=jnp.float32) + jnp.dot(p_self.astype(jnp.bfloat16), vn_head, preferred_element_type=jnp.float32)
        return (weighted / prob_sum[:, None]).astype(jnp.bfloat16)

    return lax.map(attend_head, (q_row, kn_row, vn_row, kc_row, vc_row))


def reference(hidden_in, lengths, k_cache, v_cache, ln1_gain, ln1_bias, ln2_gain, ln2_bias, w_qkv, b_qkv, w_out, b_out, w_up, b_up, w_down, b_down):
    flat_in = hidden_in.reshape(NUM_ROWS * CHUNK_LEN, D_MODEL)
    normed_attn = layer_norm(flat_in, ln1_gain, ln1_bias)
    normed_mlp = layer_norm(flat_in, ln2_gain, ln2_bias)
    qkv_all = (jnp.dot(normed_attn, w_qkv, preferred_element_type=jnp.float32) + b_qkv.astype(jnp.float32)).astype(jnp.bfloat16)
    qkv_all = qkv_all.reshape(NUM_ROWS, CHUNK_LEN, NUM_HEADS, 3, HEAD_DIM)
    positions = lengths[:, None] + jnp.arange(CHUNK_LEN, dtype=jnp.int32)[None, :]
    q_rot = jnp.swapaxes(rotary(qkv_all[:, :, :, 0], positions), 1, 2)
    k_new = jnp.swapaxes(rotary(qkv_all[:, :, :, 1], positions), 1, 2)
    v_new = jnp.swapaxes(qkv_all[:, :, :, 2], 1, 2)
    context = lax.map(attend_row, (q_rot, k_new, v_new, k_cache, v_cache, lengths))
    context = jnp.swapaxes(context, 1, 2).reshape(NUM_ROWS * CHUNK_LEN, D_MODEL)
    attn_out = jnp.dot(context, w_out, preferred_element_type=jnp.float32)
    hidden = jax.nn.gelu(jnp.dot(normed_mlp, w_up, preferred_element_type=jnp.float32) + b_up.astype(jnp.float32), approximate=False).astype(jnp.bfloat16)
    mlp_out = jnp.dot(hidden, w_down, preferred_element_type=jnp.float32)
    out_sum = flat_in.astype(jnp.float32) + attn_out + b_out.astype(jnp.float32) + mlp_out + b_down.astype(jnp.float32)
    hidden_out = out_sum.astype(jnp.bfloat16).reshape(NUM_ROWS, CHUNK_LEN, D_MODEL)
    return (hidden_out, k_new, v_new)
```

```python
import functools
import math

import jax
import jax.numpy as jnp
from jax import lax
from jax.experimental import pallas as pl
from jax.experimental.pallas import tpu as pltpu
from jax.sharding import PartitionSpec as P

EPSILON = 1e-5
NEG_BIG = -1e30
ROPE_BASE = 10000.0
ROT_DIM = 32
VMEM_LIMIT = 60 * 1024 * 1024
F32 = jnp.float32
BF16 = jnp.bfloat16
STAT_LANES = 128
SUM_LANE = 64


def params(**kw):
    return pltpu.CompilerParams(vmem_limit_bytes=VMEM_LIMIT, **kw)


def cost(flops, nbytes):
    return pl.CostEstimate(flops=int(flops), bytes_accessed=int(nbytes), transcendentals=0)


def norm_rows(x_ref, gain_ref, bias_ref, out_ref, rows):
    step = 16

    @pl.loop(0, rows // step)
    def _(i):
        at = pl.ds(pl.multiple_of(i * step, step), step)
        x = x_ref[at, :].astype(F32)
        centered = x - jnp.mean(x, axis=-1, keepdims=True)
        variance = jnp.mean(centered * centered, axis=-1, keepdims=True)
        out_ref[at, :] = (centered * lax.rsqrt(variance + EPSILON) * gain_ref[...] + bias_ref[...]).astype(BF16)


def qkv_kernel(heads, x_ref, gain_ref, bias_ref, w_ref, b_ref, cos_ref, sin_ref, q_ref, k_ref, v_ref, a_ref):
    @pl.when(pl.program_id(1) == 0)
    def _():
        norm_rows(x_ref.at[0], gain_ref, bias_ref, a_ref, a_ref.shape[0])

    lane = lax.broadcasted_iota(jnp.int32, (1, 128), 1)
    acc = jnp.dot(a_ref[...], w_ref[...], preferred_element_type=F32)
    for h in range(heads):
        for part, out in enumerate((q_ref, k_ref, v_ref)):
            col = (h * 3 + part) * 128
            val = (acc[:, col:col + 128] + b_ref[:, col:col + 128].astype(F32)).astype(BF16)
            if part < 2:
                wide = val.astype(F32)
                other = jnp.where(lane < ROT_DIM // 2, pltpu.roll(wide, 128 - ROT_DIM // 2, 1), pltpu.roll(wide, ROT_DIM // 2, 1))
                val = (wide * cos_ref[0] + other * sin_ref[0]).astype(BF16)
            out[0, h] = val


def qkv_call(hidden_in, gain, bias, w_qkv, b_qkv, cos_tab, sin_tab):
    rows, chunk, d_model = hidden_in.shape
    cols = w_qkv.shape[1]
    heads = cols // 384
    per = 2
    out = jax.ShapeDtypeStruct((rows, heads, chunk, 128), BF16)
    out_spec = pl.BlockSpec((1, per, chunk, 128), lambda m, n: (m, n, 0, 0))
    return pl.pallas_call(
        functools.partial(qkv_kernel, per),
        out_shape=(out, out, out),
        grid=(rows, heads // per),
        in_specs=[
            pl.BlockSpec((1, chunk, d_model), lambda m, n: (m, 0, 0)),
            pl.BlockSpec((1, d_model), lambda m, n: (0, 0)),
            pl.BlockSpec((1, d_model), lambda m, n: (0, 0)),
            pl.BlockSpec((d_model, per * 384), lambda m, n: (0, n)),
            pl.BlockSpec((1, per * 384), lambda m, n: (0, n)),
            pl.BlockSpec((1, chunk, 128), lambda m, n: (m, 0, 0)),
            pl.BlockSpec((1, chunk, 128), lambda m, n: (m, 0, 0)),
        ],
        out_specs=(out_spec, out_spec, out_spec),
        scratch_shapes=[pltpu.VMEM((chunk, d_model), BF16)],
        compiler_params=params(dimension_semantics=("arbitrary", "arbitrary")),
        cost_estimate=cost(2 * rows * chunk * d_model * cols, 4 * d_model * cols * 2),
        name="qkv",
    )(hidden_in, gain.reshape(1, -1), bias.reshape(1, -1), w_qkv, b_qkv.reshape(1, -1), cos_tab, sin_tab)


def flash_kernel(per, scale, block_len, idx_ref, len_ref, q_ref, kc_ref, vc_ref, kn_ref, vn_ref, ok_ref, sk_ref, os_ref, ss_ref, o_acc, m_acc, l_acc):
    row, hstep = pl.program_id(0), pl.program_id(1)
    x_id, core = idx_ref[0], idx_ref[1]
    chunk = q_ref.shape[2]
    quarter = chunk // 4
    first_slot = (x_id * 2 + core) * block_len
    valid_here = len_ref[row] - first_slot
    nsteps = pl.num_programs(1)
    do_self = jnp.logical_and(row // 2 == x_id, hstep // (nsteps // 2) == core)
    slices = (core, 2 + core, 1 - core, 3 - core)
    lane = lax.broadcasted_iota(jnp.int32, (1, STAT_LANES), 1)
    contract = (((1,), (1,)), ((), ()))

    @pl.when(hstep == 0)
    def _():
        sk_ref[...] = jnp.zeros_like(sk_ref)
        ss_ref[...] = jnp.zeros_like(ss_ref)

    def load_q(h):
        return jnp.concatenate([q_ref[0, h, pl.ds(pl.multiple_of(s * quarter, quarter), quarter), :] for s in slices], axis=0)

    def piece(q, k, v, mask):
        d = lax.dot_general(q, k, contract, preferred_element_type=F32)
        d = jnp.where(mask, d, NEG_BIG)
        top = jnp.max(d, axis=1, keepdims=True)
        p = jnp.exp2((d - top) * scale)
        return top * scale, jnp.sum(p, axis=1, keepdims=True), jnp.dot(p.astype(BF16), v, preferred_element_type=F32)

    @pl.when(valid_here <= 0)
    def _():
        o_acc[...] = jnp.zeros_like(o_acc)
        m_acc[...] = jnp.full_like(m_acc, NEG_BIG)
        l_acc[...] = jnp.zeros_like(l_acc)

    @pl.when(valid_here > 0)
    def _():
        mask = lax.broadcasted_iota(jnp.int32, (1, block_len), 1) < valid_here
        for h in range(per):
            m_acc[h], l_acc[h], o_acc[h] = piece(load_q(h), kc_ref[0, h], vc_ref[0, h], mask)

    @pl.when(do_self)
    def _():
        at = lax.broadcasted_iota(jnp.int32, (quarter, 1), 0)
        pos = jnp.concatenate([at + s * quarter for s in slices], axis=0)
        mask = pos >= lax.broadcasted_iota(jnp.int32, (1, chunk), 1)
        for h in range(per):
            m, l, o = piece(load_q(h), kn_ref[0, h], vn_ref[0, h], mask)
            top = jnp.maximum(m, m_acc[h])
            w_new, w_old = jnp.exp2(m - top), jnp.exp2(m_acc[h] - top)
            m_acc[h] = top
            l_acc[h] = l_acc[h] * w_old + l * w_new
            o_acc[h] = o_acc[h] * w_old + o * w_new

    for h in range(per):
        head = hstep * per + h
        for half, (o_ref, s_ref) in enumerate(((ok_ref, sk_ref), (os_ref, ss_ref))):
            for x in range(2):
                rows = slice((half * 2 + x) * quarter, (half * 2 + x + 1) * quarter)
                o_ref[0, x, :, h * 128:(h + 1) * 128] = o_acc[h, rows, :]
                st = jnp.where(lane == head, m_acc[h, rows, :], s_ref[0, x])
                s_ref[0, x] = jnp.where(lane == head + SUM_LANE, l_acc[h, rows, :], st)


def flash_call(index, lengths, q, k_cache, v_cache, k_new, v_new):
    rows, heads, chunk, hd = q.shape
    block_len = k_cache.shape[2]
    per = 2
    quarter = chunk // 4
    o_shape = jax.ShapeDtypeStruct((rows, 2, quarter, heads * hd), F32)
    s_shape = jax.ShapeDtypeStruct((rows, 2, quarter, STAT_LANES), F32)
    o_spec = pl.BlockSpec((1, 2, quarter, per * hd), lambda b, h, *_: (b, 0, 0, h))
    s_spec = pl.BlockSpec((1, 2, quarter, STAT_LANES), lambda b, h, *_: (b, 0, 0, 0))
    new_spec = pl.BlockSpec((1, per, chunk, hd), lambda b, h, *_: (b, h, 0, 0))
    old_spec = pl.BlockSpec((1, per, block_len, hd), lambda b, h, *_: (b, h, 0, 0))
    scale = hd ** -0.5 * math.log2(math.e)
    return pl.pallas_call(
        functools.partial(flash_kernel, per, scale, block_len),
        out_shape=(o_shape, s_shape, o_shape, s_shape),
        grid_spec=pltpu.PrefetchScalarGridSpec(
            num_scalar_prefetch=2,
            grid=(rows, heads // per),
            in_specs=[new_spec, old_spec, old_spec, new_spec, new_spec],
            out_specs=(o_spec, s_spec, o_spec, s_spec),
            scratch_shapes=[pltpu.VMEM((per, chunk, hd), F32), pltpu.VMEM((per, chunk, 1), F32), pltpu.VMEM((per, chunk, 1), F32)],
        ),
        compiler_params=params(dimension_semantics=("arbitrary", "arbitrary")),
        cost_estimate=cost(4 * rows * heads * chunk * block_len * hd * 2, rows * heads * chunk * hd * 18),
        name="flash",
    )(index, lengths, q, k_cache, v_cache, k_new, v_new)


def merge_head(h, o_a, s_a, o_b, s_b):
    cols = slice(h * 128, (h + 1) * 128)
    m_a, m_b = s_a[:, h:h + 1], s_b[:, h:h + 1]
    top = jnp.maximum(m_a, m_b)
    w_a, w_b = jnp.exp2(m_a - top), jnp.exp2(m_b - top)
    total = s_a[:, SUM_LANE + h:SUM_LANE + h + 1] * w_a + s_b[:, SUM_LANE + h:SUM_LANE + h + 1] * w_b
    return top, total, o_a[:, cols] * w_a + o_b[:, cols] * w_b


def merge_core_kernel(heads, idx_ref, oa_ref, sa_ref, ob_ref, sb_ref, om_ref, sm_ref, ot_ref, st_ref):
    lane = lax.broadcasted_iota(jnp.int32, (1, STAT_LANES), 1)
    for which, o_ref, s_ref in ((1 - idx_ref[0], ot_ref, st_ref), (idx_ref[0], om_ref, sm_ref)):
        stats = jnp.zeros(s_ref.shape[1:], F32)
        s_a, s_b = sa_ref[0, which], sb_ref[0, which]
        for h in range(heads):
            top, total, o = merge_head(h, oa_ref.at[0, which], s_a, ob_ref.at[0, which], s_b)
            o_ref[0, :, h * 128:(h + 1) * 128] = o
            stats = jnp.where(lane == h, top, stats)
            stats = jnp.where(lane == h + SUM_LANE, total, stats)
        s_ref[0] = stats


def merge_core(index, o_keep, s_keep, o_got, s_got):
    rows, _, quarter, width = o_keep.shape
    wide = pl.BlockSpec((1, 2, quarter, width), lambda b, *_: (b, 0, 0, 0))
    stat = pl.BlockSpec((1, 2, quarter, STAT_LANES), lambda b, *_: (b, 0, 0, 0))
    o_out = pl.BlockSpec((1, quarter, width), lambda b, *_: (b, 0, 0))
    s_out = pl.BlockSpec((1, quarter, STAT_LANES), lambda b, *_: (b, 0, 0))
    o_shape = jax.ShapeDtypeStruct((rows, quarter, width), F32)
    s_shape = jax.ShapeDtypeStruct((rows, quarter, STAT_LANES), F32)
    return pl.pallas_call(
        functools.partial(merge_core_kernel, width // 128),
        out_shape=(o_shape, s_shape, o_shape, s_shape),
        grid_spec=pltpu.PrefetchScalarGridSpec(num_scalar_prefetch=1, grid=(rows,), in_specs=[wide, stat, wide, stat], out_specs=(o_out, s_out, o_out, s_out)),
        compiler_params=params(dimension_semantics=("arbitrary",)),
        cost_estimate=cost(10 * o_keep.size, 12 * o_keep.size),
        name="merge_core",
    )(index, o_keep, s_keep, o_got, s_got)


def merge_x_kernel(heads, oa_ref, sa_ref, ob_ref, sb_ref, ctx_ref):
    s_a, s_b = sa_ref[0], sb_ref[0]
    for h in range(heads):
        _, total, o = merge_head(h, oa_ref.at[0], s_a, ob_ref.at[0], s_b)
        ctx_ref[0, :, h * 128:(h + 1) * 128] = (o / total).astype(BF16)


def merge_x(o_mine, s_mine, o_got, s_got):
    rows, quarter, width = o_mine.shape
    wide = pl.BlockSpec((1, quarter, width), lambda b: (b, 0, 0))
    stat = pl.BlockSpec((1, quarter, STAT_LANES), lambda b: (b, 0, 0))
    return pl.pallas_call(
        functools.partial(merge_x_kernel, width // 128),
        out_shape=jax.ShapeDtypeStruct((rows, quarter, width), BF16),
        grid=(rows,),
        in_specs=[wide, stat, wide, stat],
        out_specs=wide,
        compiler_params=params(dimension_semantics=("arbitrary",)),
        cost_estimate=cost(10 * o_mine.size, 10 * o_mine.size),
        name="merge_x",
    )(o_mine, s_mine, o_got, s_got)


def up_kernel(rows, x_ref, gain_ref, bias_ref, w_ref, b_ref, h_ref, m_ref):
    @pl.when(pl.program_id(0) == 0)
    def _():
        for r in range(rows):
            size = x_ref.shape[1]
            norm_rows(x_ref.at[r], gain_ref, bias_ref, m_ref.at[r * size:(r + 1) * size], size)

    acc = jnp.dot(m_ref[...], w_ref[...], preferred_element_type=F32) + b_ref[...].astype(F32)
    h_ref[...] = (0.5 * acc * (1.0 + lax.erf(acc * math.sqrt(0.5)))).astype(BF16)


def up_call(cp_index, hidden_in, gain, bias, w_up, b_up):
    rows, chunk, d_model = hidden_in.shape
    quarter = chunk // 4
    width = w_up.shape[1]
    tile = 512
    tokens = rows * quarter

    def body(idx_ref, *refs):
        up_kernel(rows, *refs)

    return pl.pallas_call(
        body,
        out_shape=jax.ShapeDtypeStruct((tokens, width), BF16),
        grid_spec=pltpu.PrefetchScalarGridSpec(
            num_scalar_prefetch=1,
            grid=(width // tile,),
            in_specs=[
                pl.BlockSpec((rows, quarter, d_model), lambda n, idx: (0, idx[2], 0)),
                pl.BlockSpec((1, d_model), lambda n, idx: (0, 0)),
                pl.BlockSpec((1, d_model), lambda n, idx: (0, 0)),
                pl.BlockSpec((d_model, tile), lambda n, idx: (0, n)),
                pl.BlockSpec((1, tile), lambda n, idx: (0, n)),
            ],
            out_specs=pl.BlockSpec((tokens, tile), lambda n, idx: (0, n)),
            scratch_shapes=[pltpu.VMEM((tokens, d_model), BF16)],
        ),
        compiler_params=params(dimension_semantics=("arbitrary",)),
        cost_estimate=cost(2 * tokens * d_model * width, d_model * width * 2),
        name="up",
    )(cp_index, hidden_in, gain.reshape(1, -1), bias.reshape(1, -1), w_up, b_up.reshape(1, -1))


def down_kernel(h_ref, c_ref, wd_ref, wo_ref, p_ref):
    p_ref[...] = jnp.dot(h_ref[...], wd_ref[...], preferred_element_type=F32) + jnp.dot(c_ref[...], wo_ref[...], preferred_element_type=F32)


def down_call(hidden, ctx, w_down, w_out, part, parts):
    tokens, width = hidden.shape
    inner = ctx.shape[1]
    d_model = w_down.shape[1]
    tile = 256
    cols = d_model // parts
    steps = cols // tile
    base = part * steps
    return pl.pallas_call(
        down_kernel,
        out_shape=jax.ShapeDtypeStruct((tokens, cols), F32),
        grid=(steps,),
        in_specs=[
            pl.BlockSpec((tokens, width), lambda n: (0, 0)),
            pl.BlockSpec((tokens, inner), lambda n: (0, 0)),
            pl.BlockSpec((width, tile), lambda n: (0, base + n)),
            pl.BlockSpec((inner, tile), lambda n: (0, base + n)),
        ],
        out_specs=pl.BlockSpec((tokens, tile), lambda n: (0, n)),
        compiler_params=params(dimension_semantics=("arbitrary",)),
        cost_estimate=cost(2 * tokens * (width + inner) * cols, (width + inner) * cols * 2),
        name="down",
    )(hidden, ctx, w_down, w_out)


def finish_kernel(parts, x_ref, bo_ref, bd_ref, *refs):
    out_ref = refs[-1]
    cols = refs[0].shape[2]
    for p in range(parts):
        at = slice(p * cols, (p + 1) * cols)
        total = x_ref[0, :, at].astype(F32) + refs[p][0] + bo_ref[:, at].astype(F32) + bd_ref[:, at].astype(F32)
        out_ref[0, :, at] = total.astype(BF16)


def finish_call(index, hidden_in, b_out, b_down, sums, which, out):
    rows, chunk, d_model = hidden_in.shape
    quarter = chunk // 4
    parts = len(sums)
    cols = d_model // parts
    here = pl.BlockSpec((1, quarter, d_model), lambda b, idx: (b, idx[2] ^ which, 0))
    flat = pl.BlockSpec((1, d_model), lambda b, idx: (0, 0))
    operands = [hidden_in, b_out.reshape(1, -1), b_down.reshape(1, -1)] + [s.reshape(rows, quarter, cols) for s in sums]
    in_specs = [here, flat, flat] + [pl.BlockSpec((1, quarter, cols), lambda b, idx: (b, 0, 0))] * parts
    aliases = {}
    if out is not None:
        operands.append(out)
        in_specs.append(pl.BlockSpec(memory_space=pl.ANY))
        aliases = {1 + len(operands) - 1: 0}

    def body(idx_ref, *refs):
        finish_kernel(parts, *refs)

    return pl.pallas_call(
        body,
        out_shape=jax.ShapeDtypeStruct(hidden_in.shape, BF16),
        grid_spec=pltpu.PrefetchScalarGridSpec(num_scalar_prefetch=1, grid=(rows,), in_specs=in_specs, out_specs=here),
        input_output_aliases=aliases,
        compiler_params=params(dimension_semantics=("arbitrary",)),
        cost_estimate=cost(4 * rows * quarter * d_model, rows * quarter * d_model * 8),
        name="finish",
    )(index, *operands)


def solution(mesh):
    in_specs = (P("dp", None, None), P("dp"), P("dp", "tp", "cp", None), P("dp", "tp", "cp", None), P(), P(), P(), P(), P(None, "tp"), P("tp"), P("tp", None), P(), P(None, "tp"), P("tp"), P("tp", None), P())
    out_specs = (P("dp", None, None), P("dp", "tp", None, None), P("dp", "tp", None, None))

    def swap(values, axis, bit):
        size = mesh.shape[axis]
        return jax.tree.map(lambda v: lax.ppermute(v, axis, [(i, i ^ bit) for i in range(size)]), values)

    def local_layer(hidden_in, lengths, k_block, v_block, ln1_gain, ln1_bias, ln2_gain, ln2_bias, w_qkv, b_qkv, w_out, b_out, w_up, b_up, w_down, b_down):
        rows, chunk, d_model = hidden_in.shape
        cp_index = lax.axis_index("cp")
        index = jnp.stack([cp_index // 2, cp_index % 2, cp_index]).astype(jnp.int32)

        half = ROT_DIM // 2
        inv_freq = ROPE_BASE ** (-2.0 * jnp.arange(half, dtype=F32) / ROT_DIM)
        angles = (lengths[:, None] + jnp.arange(chunk, dtype=jnp.int32)[None, :]).astype(F32)[..., None] * inv_freq
        cos, sin = jnp.cos(angles), jnp.sin(angles)
        rest = (rows, chunk, 128 - ROT_DIM)
        cos_tab = jnp.concatenate([cos, cos, jnp.ones(rest, F32)], axis=-1)
        sin_tab = jnp.concatenate([-sin, sin, jnp.zeros(rest, F32)], axis=-1)

        q, k_new, v_new = qkv_call(hidden_in, ln1_gain, ln1_bias, w_qkv, b_qkv, cos_tab, sin_tab)
        o_keep, s_keep, o_send, s_send = flash_call(index, lengths, q, k_block, v_block, k_new, v_new)
        o_got, s_got = swap((o_send, s_send), "cp", 1)
        o_mine, s_mine, o_other, s_other = merge_core(index, o_keep, s_keep, o_got, s_got)
        o_x, s_x = swap((o_other, s_other), "cp", 2)
        hidden = up_call(index, hidden_in, ln2_gain, ln2_bias, w_up, b_up)
        ctx = merge_x(o_mine, s_mine, o_x, s_x).reshape(rows * chunk // 4, -1)

        parts = 4
        own, across, beside, corner = [], [], [], []
        for part in range(parts):
            partial = down_call(hidden, ctx, w_down, w_out, part, parts)
            total = partial + swap(partial, "tp", 1)
            from_x = swap(total, "cp", 2)
            own.append(total)
            across.append(from_x)
            beside.append(swap(total, "cp", 1))
            corner.append(swap(from_x, "cp", 1))
        out = finish_call(index, hidden_in, b_out, b_down, own, 0, None)
        out = finish_call(index, hidden_in, b_out, b_down, beside, 1, out)
        out = finish_call(index, hidden_in, b_out, b_down, across, 2, out)
        out = finish_call(index, hidden_in, b_out, b_down, corner, 3, out)
        return out, k_new, v_new

    return jax.shard_map(local_layer, mesh=mesh, in_specs=in_specs, out_specs=out_specs, check_vma=False)
```
